32 devices in a mesh: sweep: 1, dp: 8 (over z, y), tensor: 4 (over x, core).
Axes of the slice: x: 2, y: 2, z: 4, core: 2. Of those that a mesh axis runs over, the one named last changes fastest.
Arguments:
- checkpoint: bfloat16 [1024, 8192], P(('sweep', 'dp'), 'tensor'), may hold values from -6 to 6
- norm_gain: bfloat16 [8192], P(('sweep', 'tensor')), may hold values from 0.5 to 1.5
- w_query: bfloat16 [8192, 4096], P(('sweep', 'dp'), 'tensor'), may hold values from -1 to 1
- w_key: bfloat16 [8192, 512], P(('sweep', 'dp'), 'tensor'), may hold values from -8 to 8
- w_value: bfloat16 [8192, 512], P(('sweep', 'dp'), 'tensor'), may hold values from -0.0625 to 0.0625
- grad_attn: bfloat16 [1024, 4096], P(('sweep', 'dp'), 'tensor'), may hold values from -6 to 6
Outputs:
- d_checkpoint: bfloat16 [1024, 8192], P(('sweep', 'dp'), 'tensor')
- grad_gain: float32 [8192], P(('sweep', 'tensor'))
- grad_query: float32 [8192, 4096], P(('sweep', 'dp'), 'tensor')
- grad_key: float32 [8192, 512], P(('sweep', 'dp'), 'tensor')
- grad_value: float32 [8192, 512], P(('sweep', 'dp'), 'tensor')
The draws below stay inside these ranges and needn't reach their ends.
All inputs are finite; a program needn't handle non-finite values.
Results may differ from the reference program's by a relative error of at most 0.025.
The reference program's roundings to bfloat16 on the way count: a program that leaves them out, or rounds other values in their place, can miss the bound.
Values may be sent and summed in bfloat16 or wider, within the bound.
No kernel may reach another device: no remote copies, remote signals or barrier semaphores. Data moves between devices by JAX's collectives and lax.ppermute only.
A program may use at most 128 MiB of HBM per device.

```python
import jax
import jax.numpy as jnp
from jax import lax

D = 8192
QHEADS = 32
KVHEADS = 4
HD = 128
TOK_DEV = 128
SEQ = 1024
N_DP = 8
N_TENSOR = 4


def query_matrix(key):
    anchor = jax.random.fold_in(key, 11)
    return jax.random.truncated_normal(anchor, -4.0, 4.0, (D, QHEADS * HD), jnp.float32) * D ** (-0.5)


def draw_w_query(key, part):
    return query_matrix(key).astype(jnp.bfloat16)


def draw_w_key(key, part):
    noise = jax.random.truncated_normal(jax.random.fold_in(key, 23), -4.0, 4.0, (D, KVHEADS * HD), jnp.float32) * D ** (-0.5)
    return noise.astype(jnp.bfloat16)


def steps_of(key, shape, split, low, high):
    def one(axis_at, shards_of):
        heights = jax.random.uniform(jax.random.fold_in(jax.random.fold_in(key, 6), axis_at), (shards_of,), jnp.float32, low / len(split), high / len(split))
        return jnp.repeat(jnp.exp(heights), shape[axis_at] // shards_of).reshape((-1,) + (1,) * (len(shape) - axis_at - 1))

    level = one(*split[0])
    for cut in split[1:]:
        level = level * one(*cut)
    return level


def gaussian(stream_key, dims, scale, most, cuts=(), kind=jnp.bfloat16):
    loudness = steps_of(stream_key, dims, cuts, -0.22, 0.18) if cuts else 1.0
    drawn = jax.random.normal(stream_key, dims, jnp.float32) * scale * loudness
    return jnp.minimum(jnp.maximum(drawn, -most), most).astype(kind)


def setup_inputs(seed: int = 0, part: int = 0) -> dict:
    streams_of = jax.random.split(jax.random.key(seed), 7)
    own_keys = jax.random.split(jax.random.fold_in(streams_of[6], part), 7)
    return {
        "checkpoint": gaussian(own_keys[0], (SEQ, D), 1.0, 6.0, ((0, 8), (1, 4))),
        "norm_gain": jnp.clip(1.0 + 0.1 * jax.random.normal(own_keys[1], (D,), jnp.float32), 0.5, 1.5).astype(jnp.bfloat16),
        "w_query": draw_w_query(jax.random.fold_in(jax.random.fold_in(streams_of[6], part), 71), part),
        "w_key": draw_w_key(jax.random.fold_in(jax.random.fold_in(streams_of[6], part), 71), part),
        "w_value": gaussian(own_keys[4], (D, KVHEADS * HD), D ** -0.5, 0.0625, ((0, 8), (1, 4))),
        "grad_attn": gaussian(own_keys[5], (SEQ, QHEADS * HD), 1.0, 6.0, ((0, 8), (1, 4))),
    }


EPS = 1e-05
THETA = 500000.0

def round_half(field):
    return lax.optimization_barrier(field.astype(jnp.bfloat16))

def angles(positions, head_width):
    frequency = THETA ** (-(jnp.arange(head_width // 2, dtype=jnp.float32) * 2.0) / head_width)
    turned = positions.astype(jnp.float32)[:, None] * frequency[None, :]
    return (jnp.cos(turned)[:, None, :], jnp.sin(turned)[:, None, :])

def rotate(field, cosine_table, sine_table):
    half_width = field.shape[-1] // 2
    front_half = field[..., :half_width]
    back_half = field[..., half_width:]
    return jnp.concatenate([front_half * cosine_table - back_half * sine_table, back_half * cosine_table + front_half * sine_table], -1)

def rotate_back(field, cosine_table, sine_table):
    half_width = field.shape[-1] // 2
    front_half = field[..., :half_width]
    back_half = field[..., half_width:]
    return jnp.concatenate([front_half * cosine_table + back_half * sine_table, back_half * cosine_table - front_half * sine_table], -1)

def reference(checkpoint, norm_gain, w_query, w_key, w_value, grad_attn):
    x_wide = checkpoint.astype(jnp.float32)
    gain_wide = norm_gain.astype(jnp.float32)
    inverse = lax.rsqrt(lax.optimization_barrier(jnp.mean(x_wide * x_wide, -1, keepdims=True)) + EPS)
    normed = (x_wide * inverse * gain_wide).astype(jnp.bfloat16)
    queries = jnp.dot(normed, w_query, preferred_element_type=jnp.float32).reshape(SEQ, QHEADS, HD)
    keyed = jnp.transpose(jnp.dot(normed, w_key, preferred_element_type=jnp.float32).reshape(SEQ, HD, KVHEADS), (0, 2, 1))
    valued = jnp.transpose(jnp.dot(normed, w_value, preferred_element_type=jnp.float32).reshape(SEQ, HD, KVHEADS), (0, 2, 1))
    cosine_table, sine_table = angles(jnp.arange(SEQ, dtype=jnp.int32), HD)
    query_rot = rotate(queries, cosine_table, sine_table).astype(jnp.bfloat16)
    key_rot = rotate(keyed, cosine_table, sine_table).astype(jnp.bfloat16)
    value_half = valued.astype(jnp.bfloat16)
    group_size = QHEADS // KVHEADS
    run_heads = min(QHEADS // N_TENSOR, group_size)
    run_count = group_size // run_heads
    score_scale = HD ** (-0.5)
    key_wide = key_rot.astype(jnp.float32)
    value_wide = value_half.astype(jnp.float32)
    upstream_all = grad_attn.reshape(SEQ, KVHEADS, group_size, HD)
    query_all = query_rot.reshape(SEQ, KVHEADS, group_size, HD)

    def attend_block(block_index):
        first_row = (block_index * TOK_DEV).astype(jnp.int32)
        query_grp = lax.dynamic_slice_in_dim(query_all, first_row, TOK_DEV, 0).astype(jnp.float32)
        upstream = lax.dynamic_slice_in_dim(upstream_all, first_row, TOK_DEV, 0).astype(jnp.float32)
        scores = jnp.einsum('tkgd,skd->kgts', query_grp, key_wide) * score_scale
        allowed = (first_row + jnp.arange(TOK_DEV, dtype=jnp.int32))[:, None] >= jnp.arange(SEQ, dtype=jnp.int32)[None, :]
        scores = jnp.where(allowed, scores, -jnp.inf)
        row_top = lax.optimization_barrier(jnp.max(scores, -1, keepdims=True))
        raw_weights = jnp.exp(scores - row_top)
        chances = raw_weights / lax.optimization_barrier(jnp.sum(raw_weights, -1, keepdims=True))
        chances_half = round_half(chances).astype(jnp.float32)
        attended = jnp.einsum('kgts,skd->tkgd', chances_half, value_wide)
        row_delta = lax.optimization_barrier(jnp.sum(upstream * attended, -1))
        prob_grads = jnp.einsum('tkgd,skd->kgts', upstream, value_wide)
        dscore = chances * (prob_grads - jnp.transpose(row_delta, (1, 2, 0))[..., None])
        dscore_half = round_half(dscore).astype(jnp.float32)
        dquery = jnp.einsum('kgts,skd->tkgd', dscore_half, key_wide) * score_scale
        dscore_runs = dscore_half.reshape(KVHEADS, run_count, run_heads, TOK_DEV, SEQ)
        chances_runs = chances_half.reshape(KVHEADS, run_count, run_heads, TOK_DEV, SEQ)
        query_runs = query_grp.reshape(TOK_DEV, KVHEADS, run_count, run_heads, HD)
        upstream_runs = upstream.reshape(TOK_DEV, KVHEADS, run_count, run_heads, HD)
        dkey_part = jnp.einsum('krgts,tkrgd->skrd', dscore_runs, query_runs) * score_scale
        dvalue_part = jnp.einsum('krgts,tkrgd->skrd', chances_runs, upstream_runs)
        return (dquery.reshape(TOK_DEV, QHEADS, HD), dkey_part.astype(jnp.bfloat16), dvalue_part.astype(jnp.bfloat16))
    dquery_all, dkey_parts, dvalue_parts = lax.map(attend_block, jnp.arange(N_DP, dtype=jnp.int32))
    dquery_all = dquery_all.reshape(SEQ, QHEADS, HD)
    dkey_sum = lax.optimization_barrier(jnp.sum(dkey_parts.astype(jnp.float32), (0, 3)))
    dvalue_sum = lax.optimization_barrier(jnp.sum(dvalue_parts.astype(jnp.float32), (0, 3)))
    dquery_pre = rotate_back(dquery_all, cosine_table, sine_table).astype(jnp.bfloat16).reshape(SEQ, QHEADS * HD)
    dkey_pre = jnp.transpose(rotate_back(dkey_sum, cosine_table, sine_table).astype(jnp.bfloat16), (0, 2, 1)).reshape(SEQ, KVHEADS * HD)
    dvalue_pre = jnp.transpose(dvalue_sum.astype(jnp.bfloat16), (0, 2, 1)).reshape(SEQ, KVHEADS * HD)
    per_query = QHEADS * HD // N_TENSOR
    per_key = KVHEADS * HD // N_TENSOR
    dnormed = jnp.zeros((SEQ, D), jnp.float32)
    for member in range(N_TENSOR):
        query_cols = slice(member * per_query, (member + 1) * per_query)
        key_cols = slice(member * per_key, (member + 1) * per_key)
        partial_term = jnp.dot(dquery_pre[:, query_cols], w_query[:, query_cols].T, preferred_element_type=jnp.float32)
        partial_term = partial_term + jnp.dot(dkey_pre[:, key_cols], w_key[:, key_cols].T, preferred_element_type=jnp.float32)
        partial_term = partial_term + jnp.dot(dvalue_pre[:, key_cols], w_value[:, key_cols].T, preferred_element_type=jnp.float32)
        dnormed = dnormed + round_half(partial_term).astype(jnp.float32)
    grad_gain = lax.optimization_barrier(jnp.sum(dnormed * x_wide * inverse, 0))
    row_sum = lax.optimization_barrier(jnp.sum(gain_wide * dnormed * x_wide, -1, keepdims=True))
    d_checkpoint = (inverse * gain_wide * dnormed - x_wide * inverse ** 3 * row_sum / D).astype(jnp.bfloat16)
    token_grads = jnp.concatenate([dquery_pre, dkey_pre, dvalue_pre], 1)

    def add_rows(running, block_index):
        first_row = (block_index * TOK_DEV).astype(jnp.int32)
        block_x = lax.dynamic_slice_in_dim(normed, first_row, TOK_DEV, 0)
        block_g = lax.dynamic_slice_in_dim(token_grads, first_row, TOK_DEV, 0)
        term = jnp.dot(block_x.T, block_g, preferred_element_type=jnp.float32)
        return (running + round_half(term).astype(jnp.float32), None)
    grads_all, unused = lax.scan(add_rows, jnp.zeros((D, (QHEADS + 2 * KVHEADS) * HD), jnp.float32), jnp.arange(N_DP, dtype=jnp.int32))
    query_width = QHEADS * HD
    key_width = KVHEADS * HD
    grad_query = grads_all[:, :query_width]
    grad_key = grads_all[:, query_width:query_width + key_width]
    grad_value = grads_all[:, query_width + key_width:]
    return (d_checkpoint, grad_gain, grad_query, grad_key, grad_value)
```

```python
import jax
import jax.numpy as jnp
from jax import lax
from jax.sharding import PartitionSpec as P

QHEADS = 32
KVHEADS = 4
HD = 128


EPS = 1e-05
THETA = 500000.0


def angles(positions, head_width):
    frequency = THETA ** (-(jnp.arange(head_width // 2, dtype=jnp.float32) * 2.0) / head_width)
    turned = positions.astype(jnp.float32)[:, None] * frequency[None, :]
    return (jnp.cos(turned)[:, None, :], jnp.sin(turned)[:, None, :])


def rotate(field, cosine_table, sine_table):
    half_width = field.shape[-1] // 2
    front_half = field[..., :half_width]
    back_half = field[..., half_width:]
    return jnp.concatenate(
        [
            front_half * cosine_table - back_half * sine_table,
            back_half * cosine_table + front_half * sine_table,
        ],
        -1,
    )


def rotate_back(field, cosine_table, sine_table):
    half_width = field.shape[-1] // 2
    front_half = field[..., :half_width]
    back_half = field[..., half_width:]
    return jnp.concatenate(
        [
            front_half * cosine_table + back_half * sine_table,
            back_half * cosine_table - front_half * sine_table,
        ],
        -1,
    )


def head_major(columns, kv_total):
    count = columns // kv_total
    source = jnp.arange(columns, dtype=jnp.int32)
    target = (source % kv_total) * count + source // kv_total
    return (target[:, None] == source[None, :]).astype(jnp.bfloat16)


def dot32(left, right):
    return jnp.dot(left, right, preferred_element_type=jnp.float32)


def spread(field, axis, size):
    copies = jnp.broadcast_to(field[None], (size,) + field.shape)
    return lax.all_to_all(copies, axis, 0, 0, tiled=True)


def make(n_dp, n_tensor):
    n_core = 2 if n_tensor % 2 == 0 else 1
    n_chip = n_tensor // n_core

    def to_core(field):
        return lax.ppermute(field, "tensor", [(m, m ^ 1) for m in range(n_tensor)])

    def to_chip(field, step):
        return lax.ppermute(
            field,
            "tensor",
            [(m, ((m // n_core + step) % n_chip) * n_core + m % n_core) for m in range(n_tensor)],
        )

    def on_device(checkpoint, norm_gain, w_query, w_key, w_value, grad_attn):
        tokens, slice_width = checkpoint.shape
        few = tokens // n_tensor
        width = slice_width * n_tensor
        rows, query_cols = w_query.shape
        kv_cols = w_key.shape[1]
        kv_total = kv_cols * n_tensor // HD
        count = kv_cols // kv_total
        group_size = QHEADS // KVHEADS
        q_heads = query_cols // HD
        own_kv = max(1, q_heads // group_size)
        run_heads = q_heads // own_kv
        seq_length = tokens * n_dp

        def heads_of(member):
            first = member * q_heads // group_size
            return range(first, first + own_kv)

        x_rows = lax.all_to_all(checkpoint, "tensor", 0, 1, tiled=True)
        gain = spread(norm_gain, "tensor", n_tensor).reshape(width).astype(jnp.float32)
        x_wide = x_rows.astype(jnp.float32)
        inverse = lax.rsqrt(jnp.mean(x_wide * x_wide, -1, keepdims=True) + EPS)
        normed = (x_wide * inverse * gain).astype(jnp.bfloat16)
        own_cols = lax.all_to_all(normed, "dp", 1, 0, tiled=True).reshape(n_dp, few, rows)
        member = lax.axis_index("tensor")
        chip, core = member // n_core, member % n_core
        arrived = [(chip, own_cols)]
        for step in range(1, n_chip):
            arrived.append(((chip + n_chip - step) % n_chip, to_chip(own_cols, step)))
        features = jnp.zeros((n_dp, n_tensor, few, rows), jnp.bfloat16)
        for source, block in arrived:
            sides = [(core, block)]
            if n_core == 2:
                sides.append((1 - core, to_core(block)))
            for side, part in sides:
                features = lax.dynamic_update_slice_in_dim(
                    features, part[:, None], source * n_core + side, 1
                )
        features = features.reshape(seq_length, rows)

        order = head_major(kv_cols, kv_total)
        w_kv = jnp.concatenate(
            [dot32(w_key, order).astype(jnp.bfloat16), dot32(w_value, order).astype(jnp.bfloat16)],
            1,
        )

        def project(left, matrix):
            part = dot32(left, matrix).astype(jnp.bfloat16)
            return part.reshape(n_dp, tokens, matrix.shape[1])

        kv_part = project(features, w_kv)
        features, kv_part = lax.optimization_barrier((features, kv_part))
        kv_part = lax.all_to_all(kv_part, "dp", 0, 0, tiled=True)
        query_part = lax.all_to_all(project(features, w_query), "dp", 0, 0, tiled=True)
        kv_local = jnp.sum(kv_part.astype(jnp.float32), 0)
        key_local, value_local = kv_local[:, :kv_cols], kv_local[:, kv_cols:]
        queries = jnp.sum(query_part.astype(jnp.float32), 0).reshape(tokens, q_heads, HD)

        first_row = lax.axis_index("dp") * tokens
        own_positions = first_row + jnp.arange(tokens, dtype=jnp.int32)
        cosine_table, sine_table = angles(own_positions, HD)

        def for_member(other):
            pieces = [
                field[:, head * count : (head + 1) * count]
                for field in (key_local, value_local)
                for head in heads_of(other)
            ]
            return jnp.concatenate(pieces, 1)

        kv_send = jnp.stack([for_member(other) for other in range(n_tensor)])
        kv_got = lax.all_to_all(kv_send, "tensor", 0, 0, tiled=True)
        kv_heads = jnp.transpose(
            kv_got.reshape(n_tensor, tokens, 2 * own_kv, count), (1, 2, 0, 3)
        ).reshape(tokens, 2 * own_kv, HD)
        key_rot = rotate(kv_heads[:, :own_kv], cosine_table, sine_table)
        kv_half = jnp.concatenate([key_rot, kv_heads[:, own_kv:]], 1).astype(jnp.bfloat16)
        kv_all = spread(kv_half.reshape(tokens, 2 * own_kv * HD), "dp", n_dp)
        kv_all = kv_all.reshape(seq_length, 2 * own_kv, HD)
        keys_three = kv_all[:, :own_kv]
        values_three = kv_all[:, own_kv:]

        query_rot = rotate(queries, cosine_table, sine_table).astype(jnp.bfloat16)
        score_scale = HD ** (-0.5)
        query_grp = query_rot.reshape(tokens, own_kv, run_heads, HD)
        upstream = grad_attn.reshape(tokens, own_kv, run_heads, HD)
        scores = (
            jnp.einsum("tkgd,skd->kgts", query_grp, keys_three, preferred_element_type=jnp.float32)
            * score_scale
        )
        allowed = own_positions[:, None] >= jnp.arange(seq_length, dtype=jnp.int32)[None, :]
        scores = jnp.where(allowed, scores, -jnp.inf)
        row_top = jnp.max(scores, -1, keepdims=True)
        raw_weights = jnp.exp(scores - row_top)
        chances = raw_weights / jnp.sum(raw_weights, -1, keepdims=True)
        chances_half = chances.astype(jnp.bfloat16)
        attended = jnp.einsum(
            "kgts,skd->tkgd", chances_half, values_three, preferred_element_type=jnp.float32
        )
        row_delta = jnp.sum(upstream.astype(jnp.float32) * attended, -1)
        prob_grads = jnp.einsum(
            "tkgd,skd->kgts", upstream, values_three, preferred_element_type=jnp.float32
        )
        dscore = chances * (prob_grads - jnp.transpose(row_delta, (1, 2, 0))[..., None])
        dscore_half = dscore.astype(jnp.bfloat16)
        dkey_part = (
            jnp.einsum("kgts,tkgd->skd", dscore_half, query_grp, preferred_element_type=jnp.float32)
            * score_scale
        )
        dvalue_part = jnp.einsum(
            "kgts,tkgd->skd", chances_half, upstream, preferred_element_type=jnp.float32
        )
        dkv_part = jnp.concatenate([dkey_part, dvalue_part], 1).astype(jnp.bfloat16)
        dkv_part = lax.all_to_all(
            dkv_part.reshape(n_dp, tokens, 2 * own_kv * HD), "dp", 0, 0, tiled=True
        )
        dkv_sum = jnp.sum(dkv_part.astype(jnp.float32), 0).reshape(tokens, 2 * own_kv, HD)
        dquery = (
            jnp.einsum("kgts,skd->tkgd", dscore_half, keys_three, preferred_element_type=jnp.float32)
            * score_scale
        )
        dkey_back = rotate_back(dkv_sum[:, :own_kv], cosine_table, sine_table)
        dkv_back = jnp.concatenate([dkey_back, dkv_sum[:, own_kv:]], 1).astype(jnp.bfloat16)
        dkv_send = jnp.transpose(
            dkv_back.reshape(tokens, 2 * own_kv, n_tensor, count), (2, 0, 1, 3)
        ).reshape(n_tensor, tokens, 2 * own_kv * count)
        dkv_got = lax.all_to_all(dkv_send, "tensor", 0, 0, tiled=True)

        def own_columns(which):
            pieces = []
            for head in range(kv_total):
                found = []
                for member in range(n_tensor):
                    for place, held in enumerate(heads_of(member)):
                        if held == head:
                            at = (which * own_kv + place) * count
                            found.append(dkv_got[member, :, at : at + count])
                if len(found) == 1:
                    pieces.append(found[0])
                else:
                    pieces.append(sum(f.astype(jnp.float32) for f in found).astype(jnp.bfloat16))
            return jnp.concatenate(pieces, 1)

        dquery_pre = (
            rotate_back(dquery.reshape(tokens, q_heads, HD), cosine_table, sine_table)
            .astype(jnp.bfloat16)
            .reshape(tokens, query_cols)
        )
        piece_q = lax.all_gather(dquery_pre, "dp", axis=0, tiled=True)
        kv_grads = jnp.concatenate([own_columns(0), own_columns(1)], 1)
        piece_kv = spread(kv_grads, "dp", n_dp).reshape(seq_length, 2 * kv_cols)

        def side_of(side):
            def rows_of(field):
                split = field.reshape(n_dp, n_chip, n_core, few, field.shape[1])
                return lax.dynamic_index_in_dim(split, side, 2, keepdims=False).reshape(
                    n_dp * n_chip * few, field.shape[1]
                )

            total = jnp.einsum(
                "tc,dc->td", rows_of(piece_q), w_query, preferred_element_type=jnp.float32
            ) + jnp.einsum("tc,dc->td", rows_of(piece_kv), w_kv, preferred_element_type=jnp.float32)
            return total.astype(jnp.bfloat16).reshape(n_dp, n_chip, few, rows)

        if n_core == 2:
            theirs = to_core(side_of(1 - core))
            halves = side_of(core).astype(jnp.float32) + theirs.astype(jnp.float32)
        else:
            halves = side_of(core).astype(jnp.float32)
        dnormed = lax.dynamic_index_in_dim(halves, chip, 1, keepdims=False)
        for step in range(1, n_chip):
            block = lax.dynamic_index_in_dim(halves, (chip + step) % n_chip, 1, keepdims=False)
            dnormed = dnormed + to_chip(block.astype(jnp.bfloat16), step).astype(jnp.float32)
        dnormed = dnormed.astype(jnp.bfloat16)
        dnormed = lax.all_to_all(dnormed, "dp", 0, 1).reshape(few, width).astype(jnp.float32)
        row_sum = jnp.sum(gain * dnormed * x_wide, -1, keepdims=True)
        d_rows = (
            inverse * gain * dnormed - x_wide * inverse**3 * row_sum / width
        ).astype(jnp.bfloat16)
        d_checkpoint = lax.all_to_all(d_rows, "tensor", 1, 0, tiled=True)
        gain_part = jnp.sum(dnormed * x_wide * inverse, 0).reshape(n_tensor, slice_width)
        gain_part = jnp.sum(lax.all_to_all(gain_part, "tensor", 0, 0, tiled=True), 0)
        grad_gain = jnp.sum(spread(gain_part, "dp", n_dp), 0)

        def weight_grad(grads):
            return jnp.einsum("td,tc->dc", features, grads, preferred_element_type=jnp.float32)

        def storage_order(grads):
            return jnp.einsum(
                "tc,dc->td", grads, order, preferred_element_type=jnp.float32
            ).astype(jnp.bfloat16)

        grad_query = weight_grad(piece_q)
        grad_key = weight_grad(storage_order(piece_kv[:, :kv_cols]))
        grad_value = weight_grad(storage_order(piece_kv[:, kv_cols:]))
        return (d_checkpoint, grad_gain, grad_query, grad_key, grad_value)

    return on_device


def solution(mesh):
    return jax.shard_map(
        make(mesh.shape["dp"], mesh.shape["tensor"]),
        mesh=mesh,
        in_specs=(
            P(("sweep", "dp"), "tensor"),
            P(("sweep", "tensor")),
            P(("sweep", "dp"), "tensor"),
            P(("sweep", "dp"), "tensor"),
            P(("sweep", "dp"), "tensor"),
            P(("sweep", "dp"), "tensor"),
        ),
        out_specs=(
            P(("sweep", "dp"), "tensor"),
            P(("sweep", "tensor")),
            P(("sweep", "dp"), "tensor"),
            P(("sweep", "dp"), "tensor"),
            P(("sweep", "dp"), "tensor"),
        ),
        check_vma=False,
    )
```

```python
import jax
import jax.numpy as jnp
from jax import lax
from jax.sharding import PartitionSpec as P

QHEADS = 32
KVHEADS = 4
HD = 128


EPS = 1e-05
THETA = 500000.0


def angles(positions, head_width):
    frequency = THETA ** (-(jnp.arange(head_width // 2, dtype=jnp.float32) * 2.0) / head_width)
    turned = positions.astype(jnp.float32)[:, None] * frequency[None, :]
    return (jnp.cos(turned)[:, None, :], jnp.sin(turned)[:, None, :])


def rotate(field, cosine_table, sine_table):
    half_width = field.shape[-1] // 2
    front_half = field[..., :half_width]
    back_half = field[..., half_width:]
    return jnp.concatenate(
        [
            front_half * cosine_table - back_half * sine_table,
            back_half * cosine_table + front_half * sine_table,
        ],
        -1,
    )


def rotate_back(field, cosine_table, sine_table):
    half_width = field.shape[-1] // 2
    front_half = field[..., :half_width]
    back_half = field[..., half_width:]
    return jnp.concatenate(
        [
            front_half * cosine_table + back_half * sine_table,
            back_half * cosine_table - front_half * sine_table,
        ],
        -1,
    )


def head_major(columns, kv_total):
    count = columns // kv_total
    source = jnp.arange(columns, dtype=jnp.int32)
    target = (source % kv_total) * count + source // kv_total
    return (target[:, None] == source[None, :]).astype(jnp.bfloat16)


def dot32(left, right):
    return jnp.dot(left, right, preferred_element_type=jnp.float32)


def spread(field, axis, size):
    copies = jnp.broadcast_to(field[None], (size,) + field.shape)
    return lax.all_to_all(copies, axis, 0, 0, tiled=True)


def shift(field, axis, size, step):
    return lax.ppermute(field, axis, [(m, (m + step) % size) for m in range(size)])


def exchange_sum(field, axis, size):
    me = lax.axis_index(axis)
    total = lax.dynamic_index_in_dim(field, me, 0, keepdims=False).astype(jnp.float32)
    for step in range(1, size):
        block = lax.dynamic_index_in_dim(field, (me + step) % size, 0, keepdims=False)
        total = total + shift(block, axis, size, step).astype(jnp.float32)
    return total


def make(n_dp, n_tensor):
    n_core = 2 if n_tensor % 2 == 0 else 1
    n_chip = n_tensor // n_core

    def to_core(field):
        return lax.ppermute(field, "tensor", [(m, m ^ 1) for m in range(n_tensor)])

    def to_chip(field, step):
        return lax.ppermute(
            field,
            "tensor",
            [(m, ((m // n_core + step) % n_chip) * n_core + m % n_core) for m in range(n_tensor)],
        )

    def on_device(checkpoint, norm_gain, w_query, w_key, w_value, grad_attn):
        tokens, slice_width = checkpoint.shape
        few = tokens // n_tensor
        width = slice_width * n_tensor
        rows, query_cols = w_query.shape
        kv_cols = w_key.shape[1]
        kv_total = kv_cols * n_tensor // HD
        count = kv_cols // kv_total
        group_size = QHEADS // KVHEADS
        q_heads = query_cols // HD
        own_kv = max(1, q_heads // group_size)
        run_heads = q_heads // own_kv
        seq_length = tokens * n_dp

        def heads_of(member):
            first = member * q_heads // group_size
            return range(first, first + own_kv)

        x_rows = lax.all_to_all(checkpoint, "tensor", 0, 1, tiled=True)
        member = lax.axis_index("tensor")
        gain = jnp.zeros((n_tensor, slice_width), jnp.bfloat16)
        for step in range(n_tensor):
            part = shift(norm_gain, "tensor", n_tensor, step) if step else norm_gain
            gain = lax.dynamic_update_slice_in_dim(
                gain, part[None], (member + n_tensor - step) % n_tensor, 0
            )
        gain = gain.reshape(width).astype(jnp.float32)
        x_wide = x_rows.astype(jnp.float32)
        inverse = lax.rsqrt(jnp.mean(x_wide * x_wide, -1, keepdims=True) + EPS)
        normed = (x_wide * inverse * gain).astype(jnp.bfloat16)
        own_cols = lax.all_to_all(normed, "dp", 1, 0, tiled=True).reshape(n_dp, few, rows)
        chip, core = member // n_core, member % n_core
        arrived = [(chip, own_cols)]
        for step in range(1, n_chip):
            arrived.append(((chip + n_chip - step) % n_chip, to_chip(own_cols, step)))
        features = jnp.zeros((n_dp, n_tensor, few, rows), jnp.bfloat16)
        for source, block in arrived:
            sides = [(core, block)]
            if n_core == 2:
                sides.append((1 - core, to_core(block)))
            for side, part in sides:
                features = lax.dynamic_update_slice_in_dim(
                    features, part[:, None], source * n_core + side, 1
                )
        features = features.reshape(seq_length, rows)

        order = head_major(kv_cols, kv_total)
        w_kv = jnp.concatenate(
            [dot32(w_key, order).astype(jnp.bfloat16), dot32(w_value, order).astype(jnp.bfloat16)],
            1,
        )

        def project(left, matrix):
            part = dot32(left, matrix).astype(jnp.bfloat16)
            return part.reshape(n_dp, tokens, matrix.shape[1])

        kv_part = project(features, w_kv)
        features, kv_part = lax.optimization_barrier((features, kv_part))
        kv_part = lax.all_to_all(kv_part, "dp", 0, 0, tiled=True)
        queries = exchange_sum(project(features, w_query), "dp", n_dp)
        kv_local = jnp.sum(kv_part.astype(jnp.float32), 0)
        key_local, value_local = kv_local[:, :kv_cols], kv_local[:, kv_cols:]
        queries = queries.reshape(tokens, q_heads, HD)

        first_row = lax.axis_index("dp") * tokens
        own_positions = first_row + jnp.arange(tokens, dtype=jnp.int32)
        cosine_table, sine_table = angles(own_positions, HD)

        def for_member(other):
            pieces = [
                field[:, head * count : (head + 1) * count]
                for field in (key_local, value_local)
                for head in heads_of(other)
            ]
            return jnp.concatenate(pieces, 1)

        kv_send = jnp.stack([for_member(other) for other in range(n_tensor)])
        kv_got = lax.all_to_all(kv_send, "tensor", 0, 0, tiled=True)
        kv_heads = jnp.transpose(
            kv_got.reshape(n_tensor, tokens, 2 * own_kv, count), (1, 2, 0, 3)
        ).reshape(tokens, 2 * own_kv, HD)
        key_rot = rotate(kv_heads[:, :own_kv], cosine_table, sine_table)
        kv_half = jnp.concatenate([key_rot, kv_heads[:, own_kv:]], 1).astype(jnp.bfloat16)
        kv_all = spread(kv_half.reshape(tokens, 2 * own_kv * HD), "dp", n_dp)
        kv_all = kv_all.reshape(seq_length, 2 * own_kv, HD)
        keys_three = kv_all[:, :own_kv]
        values_three = kv_all[:, own_kv:]

        query_rot = rotate(queries, cosine_table, sine_table).astype(jnp.bfloat16)
        score_scale = HD ** (-0.5)
        query_grp = query_rot.reshape(tokens, own_kv, run_heads, HD)
        upstream = grad_attn.reshape(tokens, own_kv, run_heads, HD)
        scores = (
            jnp.einsum("tkgd,skd->kgts", query_grp, keys_three, preferred_element_type=jnp.float32)
            * score_scale
        )
        allowed = own_positions[:, None] >= jnp.arange(seq_length, dtype=jnp.int32)[None, :]
        scores = jnp.where(allowed, scores, -jnp.inf)
        row_top = jnp.max(scores, -1, keepdims=True)
        raw_weights = jnp.exp(scores - row_top)
        chances = raw_weights / jnp.sum(raw_weights, -1, keepdims=True)
        chances_half = chances.astype(jnp.bfloat16)
        attended = jnp.einsum(
            "kgts,skd->tkgd", chances_half, values_three, preferred_element_type=jnp.float32
        )
        row_delta = jnp.sum(upstream.astype(jnp.float32) * attended, -1)
        prob_grads = jnp.einsum(
            "tkgd,skd->kgts", upstream, values_three, preferred_element_type=jnp.float32
        )
        dscore = chances * (prob_grads - jnp.transpose(row_delta, (1, 2, 0))[..., None])
        dscore_half = dscore.astype(jnp.bfloat16)
        dkey_part = (
            jnp.einsum("kgts,tkgd->skd", dscore_half, query_grp, preferred_element_type=jnp.float32)
            * score_scale
        )
        dvalue_part = jnp.einsum(
            "kgts,tkgd->skd", chances_half, upstream, preferred_element_type=jnp.float32
        )
        dkv_part = jnp.concatenate([dkey_part, dvalue_part], 1).astype(jnp.bfloat16)
        dkv_part = lax.all_to_all(
            dkv_part.reshape(n_dp, tokens, 2 * own_kv * HD), "dp", 0, 0, tiled=True
        )
        dkv_sum = jnp.sum(dkv_part.astype(jnp.float32), 0).reshape(tokens, 2 * own_kv, HD)
        dquery = (
            jnp.einsum("kgts,skd->tkgd", dscore_half, keys_three, preferred_element_type=jnp.float32)
            * score_scale
        )
        dkey_back = rotate_back(dkv_sum[:, :own_kv], cosine_table, sine_table)
        dkv_back = jnp.concatenate([dkey_back, dkv_sum[:, own_kv:]], 1).astype(jnp.bfloat16)
        dkv_send = jnp.transpose(
            dkv_back.reshape(tokens, 2 * own_kv, n_tensor, count), (2, 0, 1, 3)
        ).reshape(n_tensor, tokens, 2 * own_kv * count)
        dkv_got = lax.all_to_all(dkv_send, "tensor", 0, 0, tiled=True)

        def own_columns(which):
            pieces = []
            for head in range(kv_total):
                found = []
                for member in range(n_tensor):
                    for place, held in enumerate(heads_of(member)):
                        if held == head:
                            at = (which * own_kv + place) * count
                            found.append(dkv_got[member, :, at : at + count])
                if len(found) == 1:
                    pieces.append(found[0])
                else:
                    pieces.append(sum(f.astype(jnp.float32) for f in found).astype(jnp.bfloat16))
            return jnp.concatenate(pieces, 1)

        dquery_pre = (
            rotate_back(dquery.reshape(tokens, q_heads, HD), cosine_table, sine_table)
            .astype(jnp.bfloat16)
            .reshape(tokens, query_cols)
        )
        piece_q = lax.all_gather(dquery_pre, "dp", axis=0, tiled=True)
        kv_grads = jnp.concatenate([own_columns(0), own_columns(1)], 1)
        piece_kv = spread(kv_grads, "dp", n_dp).reshape(seq_length, 2 * kv_cols)

        def side_of(side):
            def rows_of(field):
                split = field.reshape(n_dp, n_chip, n_core, few, field.shape[1])
                return lax.dynamic_index_in_dim(split, side, 2, keepdims=False).reshape(
                    n_dp * n_chip * few, field.shape[1]
                )

            total = jnp.einsum(
                "tc,dc->td", rows_of(piece_q), w_query, preferred_element_type=jnp.float32
            ) + jnp.einsum("tc,dc->td", rows_of(piece_kv), w_kv, preferred_element_type=jnp.float32)
            return total.astype(jnp.bfloat16).reshape(n_dp, n_chip, few, rows)

        if n_core == 2:
            theirs = to_core(side_of(1 - core))
            halves = side_of(core).astype(jnp.float32) + theirs.astype(jnp.float32)
        else:
            halves = side_of(core).astype(jnp.float32)
        dnormed = lax.dynamic_index_in_dim(halves, chip, 1, keepdims=False)
        for step in range(1, n_chip):
            block = lax.dynamic_index_in_dim(halves, (chip + step) % n_chip, 1, keepdims=False)
            dnormed = dnormed + to_chip(block.astype(jnp.bfloat16), step).astype(jnp.float32)
        def weight_grad(grads):
            return jnp.einsum("td,tc->dc", features, grads, preferred_element_type=jnp.float32)

        dnormed, grad_query = lax.optimization_barrier(
            (dnormed.astype(jnp.bfloat16), weight_grad(piece_q))
        )
        dnormed = lax.all_to_all(dnormed, "dp", 0, 1).reshape(few, width).astype(jnp.float32)
        row_sum = jnp.sum(gain * dnormed * x_wide, -1, keepdims=True)
        d_rows = (
            inverse * gain * dnormed - x_wide * inverse**3 * row_sum / width
        ).astype(jnp.bfloat16)
        d_checkpoint = lax.all_to_all(d_rows, "tensor", 1, 0, tiled=True)
        gain_part = jnp.sum(dnormed * x_wide * inverse, 0).reshape(n_tensor, slice_width)
        gain_part = exchange_sum(gain_part, "tensor", n_tensor)
        place = lax.axis_index("dp")
        gain_all = jnp.zeros((n_dp, slice_width), jnp.float32)
        for step in range(n_dp):
            part = shift(gain_part, "dp", n_dp, step) if step else gain_part
            gain_all = lax.dynamic_update_slice_in_dim(
                gain_all, part[None], (place + n_dp - step) % n_dp, 0
            )
        grad_gain = jnp.sum(gain_all, 0)

        def storage_order(grads):
            return jnp.einsum(
                "tc,dc->td", grads, order, preferred_element_type=jnp.float32
            ).astype(jnp.bfloat16)

        grad_key = weight_grad(storage_order(piece_kv[:, :kv_cols]))
        grad_value = weight_grad(storage_order(piece_kv[:, kv_cols:]))
        return (d_checkpoint, grad_gain, grad_query, grad_key, grad_value)

    return on_device


def solution(mesh):
    return jax.shard_map(
        make(mesh.shape["dp"], mesh.shape["tensor"]),
        mesh=mesh,
        in_specs=(
            P(("sweep", "dp"), "tensor"),
            P(("sweep", "tensor")),
            P(("sweep", "dp"), "tensor"),
            P(("sweep", "dp"), "tensor"),
            P(("sweep", "dp"), "tensor"),
            P(("sweep", "dp"), "tensor"),
        ),
        out_specs=(
            P(("sweep", "dp"), "tensor"),
            P(("sweep", "tensor")),
            P(("sweep", "dp"), "tensor"),
            P(("sweep", "dp"), "tensor"),
            P(("sweep", "dp"), "tensor"),
        ),
        check_vma=False,
    )
```
